128 devices in a mesh: band: 8 (over y, x_lo), chan: 16 (over x_hi, z, core).
Axes of the slice: x: 4 (x_hi: 2, x_lo: 2; x = x_hi * 2 + x_lo), y: 4, z: 4, core: 2. Of those that a mesh axis runs over, the one named last changes fastest.
Arguments:
- coeffs: bfloat16 [2, 8, 1024, 8192], P(None, None, 'chan', 'band'), may hold values from -1100 to 1100, as said below
Outputs:
- coherence: float32 [1024, 1024], P('chan', 'band')
The draws below stay inside these ranges and needn't reach their ends.
Inputs may be any that keep to these rules, and one draw needn't show every extreme that they name: `coeffs`: finite real and imaginary parts.
All inputs are finite; a program needn't handle non-finite values.
Results may differ from the reference program's by a relative error of at most 0.0003.
Values may be sent and summed in bfloat16 or wider, within the bound.
A program may use at most 192 MiB of HBM per device.

```python
import jax
import jax.numpy as jnp
from jax import lax

C = 1024
K = 8
W = 16
BINS = 8192


def draw_coeffs(key, part):
    noise_key = jax.random.fold_in(jax.random.fold_in(key, 17), 0)
    noise = jnp.clip(jax.random.normal(noise_key, (2, K, C, BINS), jnp.float32), -6.0, 6.0)
    values = noise
    return values.astype(jnp.bfloat16)


def setup_inputs(seed: int = 0) -> dict:
    splits = jax.random.split(jax.random.key(seed), 2)
    return {
        "coeffs": draw_coeffs(jax.random.fold_in(splits[1], 71), 0),
    }


epsilon = 1e-6


def band_term(total, block):
    width = block.shape[2]
    flat = block.transpose(2, 0, 1, 3).reshape(width, -1)
    paired = jnp.stack((block[1], -block[0]), axis=0).transpose(2, 0, 1, 3).reshape(width, -1)
    real_part = jnp.dot(flat, flat.T, preferred_element_type=jnp.float32)
    imag_part = jnp.dot(paired, flat.T, preferred_element_type=jnp.float32)
    wide = flat.astype(jnp.float32)
    power = jnp.sum(wide * wide, axis=1) + epsilon
    coh_band = (real_part * real_part + imag_part * imag_part) / (power[:, None] * power[None, :])
    return total + coh_band, None


def reference(coeffs):
    num_bands = BINS // W
    width = coeffs.shape[2]
    blocks = coeffs.reshape(2, K, width, num_bands, W)
    blocks = jnp.moveaxis(blocks, 3, 0)
    total, unused = lax.scan(band_term, jnp.zeros((width, width), jnp.float32), blocks)
    rows = lax.broadcasted_iota(jnp.int32, (width, width), 0)
    cols = lax.broadcasted_iota(jnp.int32, (width, width), 1)
    total = jnp.where(rows == cols, jnp.float32(0.0), total)
    return total * jnp.float32(W * K / num_bands)
```

```python
import jax
import jax.numpy as jnp
from jax import lax
from jax.experimental import pallas as pl
from jax.experimental.pallas import tpu as pltpu
from jax.sharding import PartitionSpec as P

W = 16
CHUNKS = 2

epsilon = 1e-06

MESH = pl.DeviceIdType.MESH

PARTS = ((0, 24, "xyz"), (24, 48, "yzx"), (48, 64, "zxy"))


def kernel(
    x_ref, out_ref, win, snd, xb, inv_col, inv_row, pa, pb, pc, ra1, rb1, rc1, ra2, rb2, rc2, ra3, rb3, rc3,
    load_sem, send_sem, recv_sem, pass_sem, passed_sem, out_sem, in_sem,
):
    band = lax.axis_index("band")
    chan = lax.axis_index("chan")
    core = chan % 2
    z = (chan // 2) % 4
    x_hi = chan // 8
    y = band // 2
    x = x_hi * 2 + band % 2
    me = x_hi * 4 + z
    bands, chips, cores, own, depth = xb.shape
    half = depth // 2
    tapers = half // W
    step = bands // CHUNKS

    def device(x, y, z, core):
        return {"band": y * 2 + x % 2, "chan": ((x // 2) * 4 + z) * 2 + core}

    def to_chip(i):
        return ((x_hi + i // 4) % 2) * 4 + (z + i % 4) % 4

    def from_chip(i):
        return ((x_hi + 2 - i // 4) % 2) * 4 + (z + 4 - i % 4) % 4

    def same_group(chip):
        return {"band": band, "chan": chip * 2 + core}

    sibling = {"band": band, "chan": me * 2 + 1 - core}

    barrier = pltpu.get_barrier_semaphore()
    peers = [same_group(to_chip(i)) for i in range(1, 8)] + [sibling]
    peers += [device((x + o) % 4, y, z, core) for o in (1, 3)]
    peers += [device(x, (y + o) % 4, z, core) for o in (1, 2, 3)]
    for peer in peers:
        pl.semaphore_signal(barrier, inc=1, device_id=peer, device_id_type=MESH)

    def load(i):
        chip = to_chip(i)
        lanes = pl.ds(pl.multiple_of(chip * 128, 128), 128)
        return pltpu.make_async_copy(x_ref.at[:, :, :, lanes], win.at[i], load_sem.at[i])

    for i in range(chips):
        load(i).start()

    lane_band = lax.broadcasted_iota(jnp.int32, (16, 128), 1) // W

    def transposed(i, put):
        for part in range(2):
            for r in range(0, own, 16):
                v = [win[i, part, k, r : r + 16, :].astype(jnp.float32) for k in range(tapers)]
                bit = 1
                while bit < tapers:
                    upper = (lane_band // bit) % 2 == 1
                    for a in range(tapers):
                        if not a & bit:
                            b = a | bit
                            up = pltpu.roll(v[b], W * bit, 1)
                            down = pltpu.roll(v[a], 128 - W * bit, 1)
                            v[a], v[b] = jnp.where(upper, up, v[a]), jnp.where(upper, v[b], down)
                    bit *= 2
                for b in range(bands):
                    put(b, r, part, v[b].astype(jnp.bfloat16))

    load(0).wait()

    def put_own(b, r, part, value):
        xb[b, me, core, r : r + 16, part * half : (part + 1) * half] = value

    transposed(0, put_own)

    def relayout(j, carry):
        i = chips - 1 - j
        load(i).wait()

        def put(b, r, part, value):
            snd[i, b, r : r + 16, part * half : (part + 1) * half] = value

        transposed(i, put)
        return carry

    lax.fori_loop(0, chips - 1, relayout, 0)

    def send(i, c):
        return pltpu.make_async_remote_copy(
            src_ref=snd.at[i, pl.ds(c * step, step)],
            dst_ref=xb.at[pl.ds(c * step, step), me, core],
            send_sem=send_sem.at[i, c],
            recv_sem=recv_sem.at[i, c],
            device_id=same_group(to_chip(i)),
            device_id_type=MESH,
        )

    def forward(i, c):
        chip = from_chip(i)
        return pltpu.make_async_remote_copy(
            src_ref=xb.at[pl.ds(c * step, step), chip, core],
            dst_ref=xb.at[pl.ds(c * step, step), chip, core],
            send_sem=pass_sem.at[i, c],
            recv_sem=passed_sem.at[i, c],
            device_id=sibling,
            device_id_type=MESH,
        )

    pl.semaphore_wait(barrier, len(peers))
    for c in range(CHUNKS):
        def start_send(j, carry):
            send(chips - 1 - j, c).start()
            return carry

        lax.fori_loop(0, chips - 1, start_send, 0)
        forward(0, c).start()

    lane = lax.broadcasted_iota(jnp.int32, (2 * own, 128), 1)

    def normalise(i, c):
        forward(i, c).wait_recv()
        chip = from_chip(i)
        power = jnp.ones((2 * own, 128), jnp.float32)
        for b in range(step):
            v = xb[c * step + b, chip].reshape(2 * own, depth).astype(jnp.float32)
            v = v * v
            total = jnp.sum(v[:, :half] + v[:, half:], axis=1, keepdims=True) + epsilon
            power = jnp.where(lane == b, total, power)
        inverse = 1.0 / power
        inv_col[c, pl.ds(pl.multiple_of(chip * 2 * own, 128), 2 * own), :] = inverse
        inv_row[c, :, pl.ds(pl.multiple_of(chip * 128, 128), 128)] = inverse.T[:8, :]

    contract = (((1,), (1,)), ((), ()))
    stores = ((pa, 0), (pb, 1), (pc, 2))

    for c in range(CHUNKS):
        def arrive(j, carry):
            i = chips - 1 - j
            send(i, c).wait_recv()
            forward(i, c).start()
            normalise((i + 1) % chips, c)
            return carry

        lax.fori_loop(0, chips - 1, arrive, 0)
        normalise(1, c)

        def tile(t, carry):
            row = t // 4
            col = t % 4
            acc = jnp.zeros((256, 256), jnp.float32)
            scale_row = inv_row[c, :, pl.ds(pl.multiple_of(col * 256, 256), 256)]
            for b in range(step):
                left = xb[c * step + b, pl.ds(row * 4, 4), core].reshape(256, depth)
                right = xb[c * step + b, pl.ds(col * 2, 2)].reshape(256, depth)
                turned = jnp.concatenate([left[:, half:], -left[:, :half]], axis=1)
                re = lax.dot_general(left, right, contract, preferred_element_type=jnp.float32)
                im = lax.dot_general(turned, right, contract, preferred_element_type=jnp.float32)
                rows = jnp.concatenate(
                    [
                        inv_col[c, pl.ds(pl.multiple_of((row * 4 + q) * 128 + core * own, own), own), b : b + 1]
                        for q in range(4)
                    ],
                    axis=0,
                )
                acc += ((re * re + im * im) * rows) * scale_row[b : b + 1, :]
            for q in range(4):
                for s in range(2):
                    for ref, n in stores:
                        low, high, order = PARTS[n]
                        at = {"x": row * 2 + s, "y": col, "z": q}
                        index = tuple(at[d] for d in order)
                        value = acc[q * 64 + low : q * 64 + high, s * 128 : (s + 1) * 128]
                        if c > 0:
                            value = value + ref[index]
                        ref[index] = value
            return carry

        lax.fori_loop(0, 8, tile, 0)

    at = {"x": x, "y": y, "z": z}

    def hop(n, phase, o):
        low, high, order = PARTS[n]
        dim = order[phase]
        there = dict(at)
        there[dim] = (at[dim] + o) % 4
        src = stores[n][0]
        for d in order[:phase]:
            src = src.at[at[d]]
        return pltpu.make_async_remote_copy(
            src_ref=src.at[there[dim]],
            dst_ref=((ra1, rb1, rc1), (ra2, rb2, rc2), (ra3, rb3, rc3))[phase][n].at[o - 1],
            send_sem=out_sem.at[n, phase, o],
            recv_sem=in_sem.at[n, phase, o],
            device_id=device(there["x"], there["y"], there["z"], core),
            device_id_type=MESH,
        )

    for n in range(3):
        for o in (2, 1, 3):
            hop(n, 0, o).start()
    for phase in range(3):
        for n in range(3):
            low, high, order = PARTS[n]
            got = ((ra1, rb1, rc1), (ra2, rb2, rc2), (ra3, rb3, rc3))[phase][n]
            for o in (1, 3, 2):
                hop(n, phase, o).wait_recv()
            index = tuple(at[d] for d in order[: phase + 1])
            total = (stores[n][0][index] + got[0]) + (got[1] + got[2])
            if phase < 2:
                stores[n][0][index] = total
                for o in (2, 1, 3):
                    hop(n, phase + 1, o).start()
            else:
                groups = lax.axis_size("band")
                scale = jnp.float32(W * tapers / (bands * chips * groups))
                row = lax.broadcasted_iota(jnp.int32, (high - low, 128), 0) + (chan * own + low)
                col = lax.broadcasted_iota(jnp.int32, (high - low, 128), 1) + band * 128
                out_ref[low:high, :] = jnp.where(row == col, jnp.float32(0.0), total) * scale

    for n in range(3):
        for phase in range(3):
            for o in (1, 2, 3):
                hop(n, phase, o).wait_send()
    for c in range(CHUNKS):
        def finish(i, carry):
            send(i, c).wait_send()
            forward(i, c).wait_send()
            return carry

        lax.fori_loop(1, chips, finish, 0)
        forward(0, c).wait_send()


def body(coeffs):
    parts, tapers, own, bins = coeffs.shape
    chips = lax.axis_size("chan") // 2
    bands = 128 // W
    depth = parts * tapers * W
    rows = [high - low for low, high, _ in PARTS]
    f32 = jnp.float32
    bf16 = jnp.bfloat16
    scratch = [
        pltpu.VMEM((chips, parts, tapers, own, 128), bf16),
        pltpu.VMEM((chips, bands, own, depth), bf16),
        pltpu.VMEM((bands, chips, 2, own, depth), bf16),
        pltpu.VMEM((CHUNKS, chips * 2 * own, 128), f32),
        pltpu.VMEM((CHUNKS, 8, chips * 2 * own), f32),
    ]
    scratch += [pltpu.VMEM((4, 4, 4, r, 128), f32) for r in rows]
    scratch += [pltpu.VMEM((3, 4, 4, r, 128), f32) for r in rows]
    scratch += [pltpu.VMEM((3, 4, r, 128), f32) for r in rows]
    scratch += [pltpu.VMEM((3, r, 128), f32) for r in rows]
    scratch += [
        pltpu.SemaphoreType.DMA((chips,)),
        pltpu.SemaphoreType.DMA((chips, CHUNKS)),
        pltpu.SemaphoreType.DMA((chips, CHUNKS)),
        pltpu.SemaphoreType.DMA((chips, CHUNKS)),
        pltpu.SemaphoreType.DMA((chips, CHUNKS)),
        pltpu.SemaphoreType.DMA((3, 3, 4)),
        pltpu.SemaphoreType.DMA((3, 3, 4)),
    ]
    return pl.pallas_call(
        kernel,
        out_shape=jax.ShapeDtypeStruct((own, 128), f32),
        in_specs=[pl.BlockSpec(memory_space=pl.ANY)],
        out_specs=pl.BlockSpec(memory_space=pltpu.VMEM),
        scratch_shapes=scratch,
        compiler_params=pltpu.CompilerParams(
            collective_id=0, has_side_effects=True, vmem_limit_bytes=60 * 1024 * 1024
        ),
    )(coeffs)


def solution(mesh):
    return jax.shard_map(
        body,
        mesh=mesh,
        in_specs=(P(None, None, "chan", "band"),),
        out_specs=P("chan", "band"),
        check_vma=False,
    )
```

```python
import jax
import jax.numpy as jnp
from jax import lax
from jax.experimental import pallas as pl
from jax.experimental.pallas import tpu as pltpu
from jax.sharding import PartitionSpec as P

W = 16
CHUNKS = 1

epsilon = 1e-06

MESH = pl.DeviceIdType.MESH

PARTS = ((0, 24, "xyz"), (24, 48, "yzx"), (48, 64, "zxy"))


def kernel(
    x_ref, out_ref, win, snd, xb, inv_col, inv_row, pa, pb, pc, ra1, rb1, rc1, ra2, rb2, rc2, ra3, rb3, rc3,
    load_sem, send_sem, recv_sem, pass_sem, passed_sem, out_sem, in_sem,
):
    band = lax.axis_index("band")
    chan = lax.axis_index("chan")
    core = chan % 2
    z = (chan // 2) % 4
    x_hi = chan // 8
    y = band // 2
    x = x_hi * 2 + band % 2
    me = x_hi * 4 + z
    bands, chips, cores, own, depth = xb.shape
    half = depth // 2
    tapers = half // W
    step = bands // CHUNKS

    def device(x, y, z, core):
        return {"band": y * 2 + x % 2, "chan": ((x // 2) * 4 + z) * 2 + core}

    def to_chip(i):
        return ((x_hi + i // 4) % 2) * 4 + (z + i % 4) % 4

    def from_chip(i):
        return ((x_hi + 2 - i // 4) % 2) * 4 + (z + 4 - i % 4) % 4

    def same_group(chip):
        return {"band": band, "chan": chip * 2 + core}

    sibling = {"band": band, "chan": me * 2 + 1 - core}

    barrier = pltpu.get_barrier_semaphore()
    peers = [same_group(to_chip(i)) for i in range(1, 8)] + [sibling]
    peers += [device((x + o) % 4, y, z, core) for o in (1, 3)]
    peers += [device(x, (y + o) % 4, z, core) for o in (1, 2, 3)]
    for peer in peers:
        pl.semaphore_signal(barrier, inc=1, device_id=peer, device_id_type=MESH)

    def load(i):
        chip = to_chip(i)
        lanes = pl.ds(pl.multiple_of(chip * 128, 128), 128)
        return pltpu.make_async_copy(x_ref.at[:, :, :, lanes], win.at[i], load_sem.at[i])

    for i in range(chips):
        load(i).start()

    lane_band = lax.broadcasted_iota(jnp.int32, (16, 128), 1) // W

    def transposed(i, put):
        for part in range(2):
            for r in range(0, own, 16):
                v = [win[i, part, k, r : r + 16, :].astype(jnp.float32) for k in range(tapers)]
                bit = 1
                while bit < tapers:
                    upper = (lane_band // bit) % 2 == 1
                    for a in range(tapers):
                        if not a & bit:
                            b = a | bit
                            up = pltpu.roll(v[b], W * bit, 1)
                            down = pltpu.roll(v[a], 128 - W * bit, 1)
                            v[a], v[b] = jnp.where(upper, up, v[a]), jnp.where(upper, v[b], down)
                    bit *= 2
                for b in range(bands):
                    put(b, r, part, v[b].astype(jnp.bfloat16))

    load(0).wait()

    def put_own(b, r, part, value):
        xb[b, me, core, r : r + 16, part * half : (part + 1) * half] = value

    transposed(0, put_own)

    def relayout(j, carry):
        i = chips - 1 - j
        load(i).wait()

        def put(b, r, part, value):
            snd[i, b, r : r + 16, part * half : (part + 1) * half] = value

        transposed(i, put)
        return carry

    lax.fori_loop(0, chips - 1, relayout, 0)

    def send(i, c):
        return pltpu.make_async_remote_copy(
            src_ref=snd.at[i, pl.ds(c * step, step)],
            dst_ref=xb.at[pl.ds(c * step, step), me, core],
            send_sem=send_sem.at[i, c],
            recv_sem=recv_sem.at[i, c],
            device_id=same_group(to_chip(i)),
            device_id_type=MESH,
        )

    def forward(i, c):
        chip = from_chip(i)
        return pltpu.make_async_remote_copy(
            src_ref=xb.at[pl.ds(c * step, step), chip, core],
            dst_ref=xb.at[pl.ds(c * step, step), chip, core],
            send_sem=pass_sem.at[i, c],
            recv_sem=passed_sem.at[i, c],
            device_id=sibling,
            device_id_type=MESH,
        )

    pl.semaphore_wait(barrier, len(peers))
    for c in range(CHUNKS):
        def start_send(j, carry):
            send(chips - 1 - j, c).start()
            return carry

        lax.fori_loop(0, chips - 1, start_send, 0)
        forward(0, c).start()

    lane = lax.broadcasted_iota(jnp.int32, (2 * own, 128), 1)

    def normalise(i, c):
        forward(i, c).wait_recv()
        chip = from_chip(i)
        power = jnp.ones((2 * own, 128), jnp.float32)
        for b in range(step):
            v = xb[c * step + b, chip].reshape(2 * own, depth).astype(jnp.float32)
            v = v * v
            total = jnp.sum(v[:, :half] + v[:, half:], axis=1, keepdims=True) + epsilon
            power = jnp.where(lane == b, total, power)
        inverse = 1.0 / power
        inv_col[c, pl.ds(pl.multiple_of(chip * 2 * own, 128), 2 * own), :] = inverse
        inv_row[c, :, pl.ds(pl.multiple_of(chip * 128, 128), 128)] = inverse.T[:8, :]

    contract = (((1,), (1,)), ((), ()))
    stores = ((pa, 0), (pb, 1), (pc, 2))
    at = {"x": x, "y": y, "z": z}

    def target(dim, there):
        place = dict(at)
        place[dim] = there
        return device(place["x"], place["y"], place["z"], core)

    def hop(n, phase, o, cut=()):
        dim = PARTS[n][2][phase]
        there = (at[dim] + o) % 4
        src = stores[n][0]
        for d in PARTS[n][2][:phase]:
            src = src.at[at[d]]
        src = src.at[there]
        dst = ((ra1, rb1, rc1), (ra2, rb2, rc2), (ra3, rb3, rc3))[phase][n].at[o - 1]
        if cut:
            src, dst = src.at[cut], dst.at[cut]
        return pltpu.make_async_remote_copy(
            src_ref=src,
            dst_ref=dst,
            send_sem=out_sem.at[n, phase, o],
            recv_sem=in_sem.at[n, phase, o],
            device_id=target(dim, there),
            device_id_type=MESH,
        )

    def follow(j):
        return (chips - j) % chips

    def arrive(j, carry):
        i = follow(j)
        send(i, 0).wait_recv()
        forward(i, 0).start()
        normalise(follow(j - 1), 0)
        return carry

    lax.fori_loop(1, chips, arrive, 0)
    normalise(1, 0)

    def tile(t, carry):
        row = (x_hi + 1 + t // 4) % 2
        col = (y + 2 + 3 * (t % 4)) % 4
        acc = jnp.zeros((256, 256), jnp.float32)
        scale_row = inv_row[0, :, pl.ds(pl.multiple_of(col * 256, 256), 256)]
        for b in range(bands):
            left = xb[b, pl.ds(row * 4, 4), core].reshape(256, depth)
            right = xb[b, pl.ds(col * 2, 2)].reshape(256, depth)
            turned = jnp.concatenate([left[:, half:], -left[:, :half]], axis=1)
            re = lax.dot_general(left, right, contract, preferred_element_type=jnp.float32)
            im = lax.dot_general(turned, right, contract, preferred_element_type=jnp.float32)
            rows = jnp.concatenate(
                [
                    inv_col[0, pl.ds(pl.multiple_of((row * 4 + q) * 128 + core * own, own), own), b : b + 1]
                    for q in range(4)
                ],
                axis=0,
            )
            acc += ((re * re + im * im) * rows) * scale_row[b : b + 1, :]
        for q in range(4):
            for s in range(2):
                for ref, n in stores:
                    low, high, order = PARTS[n]
                    place = {"x": row * 2 + s, "y": col, "z": q}
                    ref[tuple(place[d] for d in order)] = acc[q * 64 + low : q * 64 + high, s * 128 : (s + 1) * 128]
        for o in range(1, 4):
            x_to = (x + o) % 4

            @pl.when(x_to // 2 == row)
            def _():
                hop(0, 0, o, (col,)).start()

            @pl.when((y + o) % 4 == col)
            def _():
                hop(1, 0, o, (slice(None), pl.ds(row * 2, 2))).start()

            hop(2, 0, o, (pl.ds(row * 2, 2), col)).start()
        return carry

    lax.fori_loop(0, 8, tile, 0)

    for phase in range(3):
        for n in range(3):
            low, high, order = PARTS[n]
            got = ((ra1, rb1, rc1), (ra2, rb2, rc2), (ra3, rb3, rc3))[phase][n]
            for o in (1, 3, 2):
                hop(n, phase, o).wait_recv()
            index = tuple(at[d] for d in order[: phase + 1])
            total = (stores[n][0][index] + got[0]) + (got[1] + got[2])
            if phase < 2:
                stores[n][0][index] = total
                for o in (2, 1, 3):
                    hop(n, phase + 1, o).start()
            else:
                groups = lax.axis_size("band")
                scale = jnp.float32(W * tapers / (bands * chips * groups))
                row = lax.broadcasted_iota(jnp.int32, (high - low, 128), 0) + (chan * own + low)
                col = lax.broadcasted_iota(jnp.int32, (high - low, 128), 1) + band * 128
                out_ref[low:high, :] = jnp.where(row == col, jnp.float32(0.0), total) * scale

    for n in range(3):
        for phase in range(3):
            for o in (1, 2, 3):
                hop(n, phase, o).wait_send()
    for c in range(CHUNKS):
        def finish(i, carry):
            send(i, c).wait_send()
            forward(i, c).wait_send()
            return carry

        lax.fori_loop(1, chips, finish, 0)
        forward(0, c).wait_send()


def body(coeffs):
    parts, tapers, own, bins = coeffs.shape
    chips = lax.axis_size("chan") // 2
    bands = 128 // W
    depth = parts * tapers * W
    rows = [high - low for low, high, _ in PARTS]
    f32 = jnp.float32
    bf16 = jnp.bfloat16
    scratch = [
        pltpu.VMEM((chips, parts, tapers, own, 128), bf16),
        pltpu.VMEM((chips, bands, own, depth), bf16),
        pltpu.VMEM((bands, chips, 2, own, depth), bf16),
        pltpu.VMEM((CHUNKS, chips * 2 * own, 128), f32),
        pltpu.VMEM((CHUNKS, 8, chips * 2 * own), f32),
    ]
    scratch += [pltpu.VMEM((4, 4, 4, r, 128), f32) for r in rows]
    scratch += [pltpu.VMEM((3, 4, 4, r, 128), f32) for r in rows]
    scratch += [pltpu.VMEM((3, 4, r, 128), f32) for r in rows]
    scratch += [pltpu.VMEM((3, r, 128), f32) for r in rows]
    scratch += [
        pltpu.SemaphoreType.DMA((chips,)),
        pltpu.SemaphoreType.DMA((chips, CHUNKS)),
        pltpu.SemaphoreType.DMA((chips, CHUNKS)),
        pltpu.SemaphoreType.DMA((chips, CHUNKS)),
        pltpu.SemaphoreType.DMA((chips, CHUNKS)),
        pltpu.SemaphoreType.DMA((3, 3, 4)),
        pltpu.SemaphoreType.DMA((3, 3, 4)),
    ]
    return pl.pallas_call(
        kernel,
        out_shape=jax.ShapeDtypeStruct((own, 128), f32),
        in_specs=[pl.BlockSpec(memory_space=pl.ANY)],
        out_specs=pl.BlockSpec(memory_space=pltpu.VMEM),
        scratch_shapes=scratch,
        compiler_params=pltpu.CompilerParams(
            collective_id=0, has_side_effects=True, vmem_limit_bytes=60 * 1024 * 1024
        ),
    )(coeffs)


def solution(mesh):
    return jax.shard_map(
        body,
        mesh=mesh,
        in_specs=(P(None, None, "chan", "band"),),
        out_specs=P("chan", "band"),
        check_vma=False,
    )
```

```python
import jax
import jax.numpy as jnp
from jax import lax
from jax.experimental import pallas as pl
from jax.experimental.pallas import tpu as pltpu
from jax.sharding import PartitionSpec as P

W = 16
CHUNKS = 1

epsilon = 1e-06

MESH = pl.DeviceIdType.MESH

PARTS = ((0, 24, "xyz"), (24, 48, "yzx"), (48, 64, "zxy"))


def kernel(
    x_ref, out_ref, win, snd, xb, inv_col, inv_row, pa, pb, pc, ra1, rb1, rc1, ra2, rb2, rc2, ra3, rb3, rc3,
    load_sem, send_sem, recv_sem, pass_sem, passed_sem, out_sem, in_sem,
):
    band = lax.axis_index("band")
    chan = lax.axis_index("chan")
    core = chan % 2
    z = (chan // 2) % 4
    x_hi = chan // 8
    y = band // 2
    x = x_hi * 2 + band % 2
    me = x_hi * 4 + z
    bands, chips, cores, own, depth = xb.shape
    half = depth // 2
    tapers = half // W
    step = bands // CHUNKS

    def device(x, y, z, core):
        return {"band": y * 2 + x % 2, "chan": ((x // 2) * 4 + z) * 2 + core}

    def to_chip(i):
        return ((x_hi + i // 4) % 2) * 4 + (z + i % 4) % 4

    def from_chip(i):
        return ((x_hi + 2 - i // 4) % 2) * 4 + (z + 4 - i % 4) % 4

    def same_group(chip):
        return {"band": band, "chan": chip * 2 + core}

    sibling = {"band": band, "chan": me * 2 + 1 - core}

    barrier = pltpu.get_barrier_semaphore()
    peers = [same_group(to_chip(i)) for i in range(1, 8)] + [sibling]
    peers += [device((x + o) % 4, y, z, core) for o in (1, 3)]
    peers += [device(x, (y + o) % 4, z, core) for o in (1, 2, 3)]
    for peer in peers:
        pl.semaphore_signal(barrier, inc=1, device_id=peer, device_id_type=MESH)

    def load(i):
        chip = to_chip(i)
        lanes = pl.ds(pl.multiple_of(chip * 128, 128), 128)
        return pltpu.make_async_copy(x_ref.at[:, :, :, lanes], win.at[i], load_sem.at[i])

    for i in range(chips):
        load(i).start()

    lane_band = lax.broadcasted_iota(jnp.int32, (16, 128), 1) // W

    def transposed(i, put):
        for part in range(2):
            for r in range(0, own, 16):
                v = [win[i, part, k, r : r + 16, :].astype(jnp.float32) for k in range(tapers)]
                bit = 1
                while bit < tapers:
                    upper = (lane_band // bit) % 2 == 1
                    for a in range(tapers):
                        if not a & bit:
                            b = a | bit
                            up = pltpu.roll(v[b], W * bit, 1)
                            down = pltpu.roll(v[a], 128 - W * bit, 1)
                            v[a], v[b] = jnp.where(upper, up, v[a]), jnp.where(upper, v[b], down)
                    bit *= 2
                for b in range(bands):
                    put(b, r, part, v[b].astype(jnp.bfloat16))

    load(0).wait()

    def put_own(b, r, part, value):
        xb[b, me, core, r : r + 16, part * half : (part + 1) * half] = value

    transposed(0, put_own)

    def relayout(j, carry):
        i = chips - 1 - j
        load(i).wait()

        def put(b, r, part, value):
            snd[i, b, r : r + 16, part * half : (part + 1) * half] = value

        transposed(i, put)
        return carry

    lax.fori_loop(0, chips - 1, relayout, 0)

    def send(i, c):
        return pltpu.make_async_remote_copy(
            src_ref=snd.at[i, pl.ds(c * step, step)],
            dst_ref=xb.at[pl.ds(c * step, step), me, core],
            send_sem=send_sem.at[i, c],
            recv_sem=recv_sem.at[i, c],
            device_id=same_group(to_chip(i)),
            device_id_type=MESH,
        )

    def forward(i, c):
        chip = from_chip(i)
        return pltpu.make_async_remote_copy(
            src_ref=xb.at[pl.ds(c * step, step), chip, core],
            dst_ref=xb.at[pl.ds(c * step, step), chip, core],
            send_sem=pass_sem.at[i, c],
            recv_sem=passed_sem.at[i, c],
            device_id=sibling,
            device_id_type=MESH,
        )

    pl.semaphore_wait(barrier, len(peers))
    for c in range(CHUNKS):
        def start_send(j, carry):
            send(chips - 1 - j, c).start()
            return carry

        lax.fori_loop(0, chips - 1, start_send, 0)
        forward(0, c).start()

    lane = lax.broadcasted_iota(jnp.int32, (2 * own, 128), 1)

    def normalise(i, c):
        forward(i, c).wait_recv()
        chip = from_chip(i)
        power = jnp.ones((2 * own, 128), jnp.float32)
        for b in range(step):
            v = xb[c * step + b, chip].reshape(2 * own, depth).astype(jnp.float32)
            v = v * v
            total = jnp.sum(v[:, :half] + v[:, half:], axis=1, keepdims=True) + epsilon
            power = jnp.where(lane == b, total, power)
        inverse = 1.0 / power
        inv_col[c, pl.ds(pl.multiple_of(chip * 2 * own, 128), 2 * own), :] = inverse
        inv_row[c, :, pl.ds(pl.multiple_of(chip * 128, 128), 128)] = inverse.T[:8, :]

    contract = (((1,), (1,)), ((), ()))
    stores = ((pa, 0), (pb, 1), (pc, 2))
    at = {"x": x, "y": y, "z": z}

    def target(dim, there):
        place = dict(at)
        place[dim] = there
        return device(place["x"], place["y"], place["z"], core)

    def hop(n, phase, o, cut=()):
        dim = PARTS[n][2][phase]
        there = (at[dim] + o) % 4
        src = stores[n][0]
        for d in PARTS[n][2][:phase]:
            src = src.at[at[d]]
        src = src.at[there]
        dst = ((ra1, rb1, rc1), (ra2, rb2, rc2), (ra3, rb3, rc3))[phase][n].at[o - 1]
        if cut:
            src, dst = src.at[cut], dst.at[cut]
        return pltpu.make_async_remote_copy(
            src_ref=src,
            dst_ref=dst,
            send_sem=out_sem.at[n, phase, o],
            recv_sem=in_sem.at[n, phase, o],
            device_id=target(dim, there),
            device_id_type=MESH,
        )

    def follow(j):
        return (chips - j) % chips

    def arrive(j, carry):
        i = follow(j)
        send(i, 0).wait_recv()
        forward(i, 0).start()
        normalise(follow(j - 1), 0)
        return carry

    lax.fori_loop(1, chips, arrive, 0)
    normalise(1, 0)

    def tile(t, carry):
        row = (x_hi + 1 + t // 4) % 2
        col = (y + 2 + 3 * (t % 4)) % 4
        acc = jnp.zeros((256, 256), jnp.float32)
        scale_row = inv_row[0, :, pl.ds(pl.multiple_of(col * 256, 256), 256)]
        for b in range(bands):
            left = xb[b, pl.ds(row * 4, 4), core].reshape(256, depth)
            right = xb[b, pl.ds(col * 2, 2)].reshape(256, depth)
            turned = jnp.concatenate([left[:, half:], -left[:, :half]], axis=1)
            re = lax.dot_general(left, right, contract, preferred_element_type=jnp.float32)
            im = lax.dot_general(turned, right, contract, preferred_element_type=jnp.float32)
            rows = jnp.concatenate(
                [
                    inv_col[0, pl.ds(pl.multiple_of((row * 4 + q) * 128 + core * own, own), own), b : b + 1]
                    for q in range(4)
                ],
                axis=0,
            )
            acc += ((re * re + im * im) * rows) * scale_row[b : b + 1, :]
        for q in range(4):
            for s in range(2):
                for ref, n in stores:
                    low, high, order = PARTS[n]
                    place = {"x": row * 2 + s, "y": col, "z": q}
                    ref[tuple(place[d] for d in order)] = acc[q * 64 + low : q * 64 + high, s * 128 : (s + 1) * 128]
        for o in range(1, 4):
            x_to = (x + o) % 4

            @pl.when(x_to // 2 == row)
            def _():
                hop(0, 0, o, (col,)).start()

            @pl.when((y + o) % 4 == col)
            def _():
                hop(1, 0, o, (slice(None), pl.ds(row * 2, 2))).start()

            hop(2, 0, o, (pl.ds(row * 2, 2), col)).start()
        return carry

    lax.fori_loop(0, 8, tile, 0)

    for phase in range(3):
        for n in range(3):
            low, high, order = PARTS[n]
            got = ((ra1, rb1, rc1), (ra2, rb2, rc2), (ra3, rb3, rc3))[phase][n]
            for o in (1, 3, 2):
                hop(n, phase, o).wait_recv()
            index = tuple(at[d] for d in order[: phase + 1])
            total = (stores[n][0][index] + got[0]) + (got[1] + got[2])
            if phase < 2:
                stores[n][0][index] = total
                for o in (2, 1, 3):
                    hop(n, phase + 1, o).start()
            else:
                groups = lax.axis_size("band")
                scale = jnp.float32(W * tapers / (bands * chips * groups))
                row = lax.broadcasted_iota(jnp.int32, (high - low, 128), 0) + (chan * own + low)
                col = lax.broadcasted_iota(jnp.int32, (high - low, 128), 1) + band * 128
                out_ref[low:high, :] = jnp.where(row == col, jnp.float32(0.0), total) * scale

    for n in range(3):
        for phase in range(3):
            for o in (1, 2, 3):
                hop(n, phase, o).wait_send()
    for c in range(CHUNKS):
        def finish(i, carry):
            send(i, c).wait_send()
            forward(i, c).wait_send()
            return carry

        lax.fori_loop(1, chips, finish, 0)
        forward(0, c).wait_send()


def body(coeffs):
    parts, tapers, own, bins = coeffs.shape
    chips = lax.axis_size("chan") // 2
    bands = 128 // W
    depth = parts * tapers * W
    rows = [high - low for low, high, _ in PARTS]
    f32 = jnp.float32
    bf16 = jnp.bfloat16
    scratch = [
        pltpu.VMEM((chips, parts, tapers, own, 128), bf16),
        pltpu.VMEM((chips, bands, own, depth), bf16),
        pltpu.VMEM((bands, chips, 2, own, depth), bf16),
        pltpu.VMEM((CHUNKS, chips * 2 * own, 128), f32),
        pltpu.VMEM((CHUNKS, 8, chips * 2 * own), f32),
    ]
    scratch += [pltpu.VMEM((4, 4, 4, r, 128), f32) for r in rows]
    scratch += [pltpu.VMEM((3, 4, 4, r, 128), f32) for r in rows]
    scratch += [pltpu.VMEM((3, 4, r, 128), f32) for r in rows]
    scratch += [pltpu.VMEM((3, r, 128), f32) for r in rows]
    scratch += [
        pltpu.SemaphoreType.DMA((chips,)),
        pltpu.SemaphoreType.DMA((chips, CHUNKS)),
        pltpu.SemaphoreType.DMA((chips, CHUNKS)),
        pltpu.SemaphoreType.DMA((chips, CHUNKS)),
        pltpu.SemaphoreType.DMA((chips, CHUNKS)),
        pltpu.SemaphoreType.DMA((3, 3, 4)),
        pltpu.SemaphoreType.DMA((3, 3, 4)),
    ]
    return pl.pallas_call(
        kernel,
        out_shape=jax.ShapeDtypeStruct((own, 128), f32),
        in_specs=[pl.BlockSpec(memory_space=pl.ANY)],
        out_specs=pl.BlockSpec(memory_space=pltpu.VMEM),
        scratch_shapes=scratch,
        compiler_params=pltpu.CompilerParams(
            collective_id=0, has_side_effects=True, vmem_limit_bytes=54000 * 1024
        ),
    )(coeffs)


def solution(mesh):
    return jax.shard_map(
        body,
        mesh=mesh,
        in_specs=(P(None, None, "chan", "band"),),
        out_specs=P("chan", "band"),
        check_vma=False,
    )
```

```python
import jax
import jax.numpy as jnp
from jax import lax
from jax.experimental import pallas as pl
from jax.experimental.pallas import tpu as pltpu
from jax.sharding import PartitionSpec as P

W = 16

SENDS = (6, 2, 5, 1, 7, 3, 4)
EVENTS = (-6, 2, -5, 1, 3, (0, 2, 1, 3), -7, 6, 5, 7, 4, (6, 5, 7, 4))

epsilon = 1e-06

MESH = pl.DeviceIdType.MESH

PARTS = ((0, 24, "xyz"), (24, 40, "yzx"), (40, 64, "zxy"))


def kernel(
    x_ref, out_ref, win, snd, mid, xb, inv_col, inv_row, pa, pb, pc, ra1, rb1, rc1, ra2, rb2, rc2, ra3, rb3, rc3,
    load_sem, send_sem, recv_sem, mid_in, mid_out, pass_sem, passed_sem, out_sem, in_sem,
):
    band = lax.axis_index("band")
    chan = lax.axis_index("chan")
    core = chan % 2
    z = (chan // 2) % 4
    x_hi = chan // 8
    y = band // 2
    x = x_hi * 2 + band % 2
    me = x_hi * 4 + z
    bands, chips, cores, own, depth = xb.shape
    half = depth // 2
    tapers = half // W

    def device(x, y, z, core):
        return {"band": y * 2 + x % 2, "chan": ((x // 2) * 4 + z) * 2 + core}

    def pick(table, j):
        return sum(v * (1 - jnp.minimum(jnp.abs(j - n), 1)) for n, v in enumerate(table))

    def to_chip(i):
        return ((x_hi + i // 4) % 2) * 4 + (z + i % 4) % 4

    def from_chip(i):
        return ((x_hi + 2 - i // 4) % 2) * 4 + (z + 4 - i % 4) % 4

    def same_group(chip):
        return {"band": band, "chan": chip * 2 + core}

    sibling = {"band": band, "chan": me * 2 + 1 - core}

    barrier = pltpu.get_barrier_semaphore()
    peers = [sibling] + [device((x + o) % 4, y, z, core) for o in (1, 2, 3)]
    peers += [device(x, (y + o) % 4, z, core) for o in (1, 2, 3)]
    peers += [device(x, y, (z + o) % 4, core) for o in (1, 2, 3)]
    for peer in peers:
        pl.semaphore_signal(barrier, inc=1, device_id=peer, device_id_type=MESH)

    def load(i):
        chip = to_chip(i)
        lanes = pl.ds(pl.multiple_of(chip * 128, 128), 128)
        return pltpu.make_async_copy(x_ref.at[:, :, :, lanes], win.at[i], load_sem.at[i])

    for i in SENDS + (0,):
        load(i).start()

    lane_band = lax.broadcasted_iota(jnp.int32, (16, 128), 1) // W

    def transposed(i, put):
        for part in range(2):
            for r in range(0, own, 16):
                v = [win[i, part, k, r : r + 16, :].astype(jnp.float32) for k in range(tapers)]
                bit = 1
                while bit < tapers:
                    upper = (lane_band // bit) % 2 == 1
                    for a in range(tapers):
                        if not a & bit:
                            b = a | bit
                            up = pltpu.roll(v[b], W * bit, 1)
                            down = pltpu.roll(v[a], 128 - W * bit, 1)
                            v[a], v[b] = jnp.where(upper, up, v[a]), jnp.where(upper, v[b], down)
                    bit *= 2
                for b in range(bands):
                    put(b, r, part, v[b].astype(jnp.bfloat16))

    def relayout(i):
        load(i).wait()

        def put(b, r, part, value):
            snd[i, b, r : r + 16, part * half : (part + 1) * half] = value

        transposed(i, put)

    across = device((x + 2) % 4, y, z, core)

    def along(dz):
        return device(x, y, (z + dz) % 4, core)

    def send(i):
        return pltpu.make_async_remote_copy(
            src_ref=snd.at[i],
            dst_ref=xb.at[:, me, core],
            send_sem=send_sem.at[i],
            recv_sem=recv_sem.at[i],
            device_id=device((x + 2 * (i // 4)) % 4, y, (z + i % 4) % 4, core),
            device_id_type=MESH,
        )

    def to_mid(i):
        return pltpu.make_async_remote_copy(
            src_ref=snd.at[i],
            dst_ref=mid.at[i - 4],
            send_sem=send_sem.at[i],
            recv_sem=mid_in.at[i - 4],
            device_id=across,
            device_id_type=MESH,
        )

    def from_mid(i):
        return pltpu.make_async_remote_copy(
            src_ref=mid.at[i - 4],
            dst_ref=xb.at[:, (1 - x_hi) * 4 + z, core],
            send_sem=mid_out.at[i - 4],
            recv_sem=recv_sem.at[i],
            device_id=along(i - 4),
            device_id_type=MESH,
        )

    def landed(i):
        return send(i) if i <= 4 else from_mid(i)

    def forward(i):
        chip = from_chip(i)
        return pltpu.make_async_remote_copy(
            src_ref=xb.at[:, chip, core],
            dst_ref=xb.at[:, chip, core],
            send_sem=pass_sem.at[i],
            recv_sem=passed_sem.at[i],
            device_id=sibling,
            device_id_type=MESH,
        )

    relayout(SENDS[0])
    pl.semaphore_wait(barrier, len(peers))
    to_mid(SENDS[0]).start()

    def relayout_and_send(j, carry):
        i = pick(SENDS, j)
        relayout(i)

        @pl.when(i > 4)
        def _():
            to_mid(i).start()

        @pl.when(i <= 4)
        def _():
            send(i).start()

        return carry

    lax.fori_loop(1, chips - 1, relayout_and_send, 0)
    load(0).wait()

    def put_own(b, r, part, value):
        xb[b, me, core, r : r + 16, part * half : (part + 1) * half] = value

    transposed(0, put_own)
    forward(0).start()

    lane = lax.broadcasted_iota(jnp.int32, (2 * own, 128), 1)

    def normalise(i):
        forward(i).wait_recv()
        chip = from_chip(i)
        power = jnp.ones((2 * own, 128), jnp.float32)
        for b in range(bands):
            v = xb[b, chip].reshape(2 * own, depth).astype(jnp.float32)
            v = v * v
            total = jnp.sum(v[:, :half] + v[:, half:], axis=1, keepdims=True) + epsilon
            power = jnp.where(lane == b, total, power)
        inverse = 1.0 / power
        inv_col[pl.ds(pl.multiple_of(chip * 2 * own, 128), 2 * own), :] = inverse
        inv_row[:, pl.ds(pl.multiple_of(chip * 128, 128), 128)] = inverse.T[:8, :]

    contract = (((1,), (1,)), ((), ()))
    stores = ((pa, 0), (pb, 1), (pc, 2))
    at = {"x": x, "y": y, "z": z}

    def target(dim, there):
        place = dict(at)
        place[dim] = there
        return device(place["x"], place["y"], place["z"], core)

    def hop(n, phase, o, cut=()):
        dim = PARTS[n][2][phase]
        there = (at[dim] + o) % 4
        src = stores[n][0]
        for d in PARTS[n][2][:phase]:
            src = src.at[at[d]]
        src = src.at[there]
        dst = ((ra1, rb1, rc1), (ra2, rb2, rc2), (ra3, rb3, rc3))[phase][n].at[o - 1]
        if cut:
            src, dst = src.at[cut], dst.at[cut]
        return pltpu.make_async_remote_copy(
            src_ref=src,
            dst_ref=dst,
            send_sem=out_sem.at[n, phase, o],
            recv_sem=in_sem.at[n, phase, o],
            device_id=target(dim, there),
            device_id_type=MESH,
        )

    def group(items):
        def one(j, carry):
            normalise(pick(items, j))
            return carry

        lax.fori_loop(0, len(items), one, 0)

    for event in EVENTS:
        if isinstance(event, tuple):
            group(event)
        elif event < 0:
            to_mid(-event).wait_recv()
            from_mid(-event).start()
        else:
            landed(event).wait_recv()
            forward(event).start()

    def tile(t, carry):
        row = (x_hi + 1 + t // 4) % 2
        col = (y + 2 + 3 * (t % 4)) % 4
        acc = jnp.zeros((256, 256), jnp.float32)
        scale_row = inv_row[:, pl.ds(pl.multiple_of(col * 256, 256), 256)]
        for b in range(bands):
            left = xb[b, pl.ds(row * 4, 4), core].reshape(256, depth)
            right = xb[b, pl.ds(col * 2, 2)].reshape(256, depth)
            turned = jnp.concatenate([left[:, half:], -left[:, :half]], axis=1)
            re = lax.dot_general(left, right, contract, preferred_element_type=jnp.float32)
            im = lax.dot_general(turned, right, contract, preferred_element_type=jnp.float32)
            rows = jnp.concatenate(
                [
                    inv_col[pl.ds(pl.multiple_of((row * 4 + q) * 128 + core * own, own), own), b : b + 1]
                    for q in range(4)
                ],
                axis=0,
            )
            acc += ((re * re + im * im) * rows) * scale_row[b : b + 1, :]
        for q in range(4):
            for s in range(2):
                for ref, n in stores:
                    low, high, order = PARTS[n]
                    place = {"x": row * 2 + s, "y": col, "z": q}
                    ref[tuple(place[d] for d in order)] = acc[q * 64 + low : q * 64 + high, s * 128 : (s + 1) * 128]
        for o in range(1, 4):
            x_to = (x + o) % 4

            @pl.when(x_to // 2 == row)
            def _():
                hop(0, 0, o, (col,)).start()

            @pl.when((y + o) % 4 == col)
            def _():
                hop(1, 0, o, (slice(None), pl.ds(row * 2, 2))).start()

            hop(2, 0, o, (pl.ds(row * 2, 2), col)).start()
        return carry

    lax.fori_loop(0, 8, tile, 0)

    for phase in range(3):
        for n in range(3):
            low, high, order = PARTS[n]
            got = ((ra1, rb1, rc1), (ra2, rb2, rc2), (ra3, rb3, rc3))[phase][n]
            for o in (1, 3, 2):
                hop(n, phase, o).wait_recv()
            index = tuple(at[d] for d in order[: phase + 1])
            total = (stores[n][0][index] + got[0]) + (got[1] + got[2])
            if phase < 2:
                stores[n][0][index] = total
                for o in (2, 1, 3):
                    hop(n, phase + 1, o).start()
            else:
                groups = lax.axis_size("band")
                scale = jnp.float32(W * tapers / (bands * chips * groups))
                row = lax.broadcasted_iota(jnp.int32, (high - low, 128), 0) + (chan * own + low)
                col = lax.broadcasted_iota(jnp.int32, (high - low, 128), 1) + band * 128
                out_ref[low:high, :] = jnp.where(row == col, jnp.float32(0.0), total) * scale

    for n in range(3):
        for phase in range(3):
            for o in (1, 2, 3):
                hop(n, phase, o).wait_send()
    for i in range(1, 8):
        (to_mid(i) if i > 4 else send(i)).wait_send()
        forward(i).wait_send()
        if i > 4:
            from_mid(i).wait_send()
    forward(0).wait_send()


def body(coeffs):
    parts, tapers, own, bins = coeffs.shape
    chips = lax.axis_size("chan") // 2
    bands = 128 // W
    depth = parts * tapers * W
    rows = [high - low for low, high, _ in PARTS]
    f32 = jnp.float32
    bf16 = jnp.bfloat16
    scratch = [
        pltpu.VMEM((chips, parts, tapers, own, 128), bf16),
        pltpu.VMEM((chips, bands, own, depth), bf16),
        pltpu.VMEM((4, bands, own, depth), bf16),
        pltpu.VMEM((bands, chips, 2, own, depth), bf16),
        pltpu.VMEM((chips * 2 * own, 128), f32),
        pltpu.VMEM((8, chips * 2 * own), f32),
    ]
    scratch += [pltpu.VMEM((4, 4, 4, r, 128), f32) for r in rows]
    scratch += [pltpu.VMEM((3, 4, 4, r, 128), f32) for r in rows]
    scratch += [pltpu.VMEM((3, 4, r, 128), f32) for r in rows]
    scratch += [pltpu.VMEM((3, r, 128), f32) for r in rows]
    scratch += [
        pltpu.SemaphoreType.DMA((chips,)),
        pltpu.SemaphoreType.DMA((chips,)),
        pltpu.SemaphoreType.DMA((chips,)),
        pltpu.SemaphoreType.DMA((4,)),
        pltpu.SemaphoreType.DMA((4,)),
        pltpu.SemaphoreType.DMA((chips,)),
        pltpu.SemaphoreType.DMA((chips,)),
        pltpu.SemaphoreType.DMA((3, 3, 4)),
        pltpu.SemaphoreType.DMA((3, 3, 4)),
    ]
    return pl.pallas_call(
        kernel,
        out_shape=jax.ShapeDtypeStruct((own, 128), f32),
        in_specs=[pl.BlockSpec(memory_space=pl.ANY)],
        out_specs=pl.BlockSpec(memory_space=pltpu.VMEM),
        scratch_shapes=scratch,
        compiler_params=pltpu.CompilerParams(
            collective_id=0, has_side_effects=True, vmem_limit_bytes=54000 * 1024
        ),
    )(coeffs)


def solution(mesh):
    return jax.shard_map(
        body,
        mesh=mesh,
        in_specs=(P(None, None, "chan", "band"),),
        out_specs=P("chan", "band"),
        check_vma=False,
    )
```

```python
import jax
import jax.numpy as jnp
from jax import lax
from jax.experimental import pallas as pl
from jax.experimental.pallas import tpu as pltpu
from jax.sharding import PartitionSpec as P

W = 16

SENDS = (6, 2, 5, 1, 7, 3, 4)
EVENTS = (-6, 2, -5, 1, 3, (0, 2, 1, 3), -7, 6, 5, 7, 4, (6, 5, 7, 4))

epsilon = 1e-06

MESH = pl.DeviceIdType.MESH

PARTS = ((0, 24, "xyz"), (24, 40, "yzx"), (40, 64, "zxy"))


def kernel(
    x_ref, out_ref, win, snd, mid, xb, inv_col, inv_row, pa, pb, pc, ra1, rb1, rc1, ra2, rb2, rc2, ra3, rb3, rc3,
    load_sem, send_sem, recv_sem, mid_in, mid_out, pass_sem, passed_sem, out_sem, in_sem,
):
    band = lax.axis_index("band")
    chan = lax.axis_index("chan")
    core = chan % 2
    z = (chan // 2) % 4
    x_hi = chan // 8
    y = band // 2
    x = x_hi * 2 + band % 2
    me = x_hi * 4 + z
    bands, chips, cores, own, depth = xb.shape
    half = depth // 2
    tapers = half // W

    def device(x, y, z, core):
        return {"band": y * 2 + x % 2, "chan": ((x // 2) * 4 + z) * 2 + core}

    def pick(table, j):
        return sum(v * (1 - jnp.minimum(jnp.abs(j - n), 1)) for n, v in enumerate(table))

    def to_chip(i):
        return ((x_hi + i // 4) % 2) * 4 + (z + i % 4) % 4

    def from_chip(i):
        return ((x_hi + 2 - i // 4) % 2) * 4 + (z + 4 - i % 4) % 4

    def same_group(chip):
        return {"band": band, "chan": chip * 2 + core}

    sibling = {"band": band, "chan": me * 2 + 1 - core}

    def load(i):
        chip = to_chip(i)
        lanes = pl.ds(pl.multiple_of(chip * 128, 128), 128)
        return pltpu.make_async_copy(x_ref.at[:, :, :, lanes], win.at[i], load_sem.at[i])

    for i in SENDS + (0,):
        load(i).start()

    barrier = pltpu.get_barrier_semaphore()
    peers = [device((x + o) % 4, y, z, core) for o in (2, 1, 3)] + [sibling]
    peers += [device(x, (y + o) % 4, z, core) for o in (1, 2, 3)]
    peers += [device(x, y, (z + o) % 4, core) for o in (1, 2, 3)]
    for peer in peers:
        pl.semaphore_signal(barrier, inc=1, device_id=peer, device_id_type=MESH)

    lane_band = lax.broadcasted_iota(jnp.int32, (16, 128), 1) // W

    def transposed(i, put):
        for part in range(2):
            for r in range(0, own, 16):
                v = [win[i, part, k, r : r + 16, :].astype(jnp.float32) for k in range(tapers)]
                bit = 1
                while bit < tapers:
                    upper = (lane_band // bit) % 2 == 1
                    for a in range(tapers):
                        if not a & bit:
                            b = a | bit
                            up = pltpu.roll(v[b], W * bit, 1)
                            down = pltpu.roll(v[a], 128 - W * bit, 1)
                            v[a], v[b] = jnp.where(upper, up, v[a]), jnp.where(upper, v[b], down)
                    bit *= 2
                for b in range(bands):
                    put(b, r, part, v[b].astype(jnp.bfloat16))

    def relayout(i):
        load(i).wait()

        def put(b, r, part, value):
            snd[i, b, r : r + 16, part * half : (part + 1) * half] = value

        transposed(i, put)

    across = device((x + 2) % 4, y, z, core)

    def along(dz):
        return device(x, y, (z + dz) % 4, core)

    def send(i):
        return pltpu.make_async_remote_copy(
            src_ref=snd.at[i],
            dst_ref=xb.at[:, me, core],
            send_sem=send_sem.at[i],
            recv_sem=recv_sem.at[i],
            device_id=device((x + 2 * (i // 4)) % 4, y, (z + i % 4) % 4, core),
            device_id_type=MESH,
        )

    def to_mid(i):
        return pltpu.make_async_remote_copy(
            src_ref=snd.at[i],
            dst_ref=mid.at[i - 4],
            send_sem=send_sem.at[i],
            recv_sem=mid_in.at[i - 4],
            device_id=across,
            device_id_type=MESH,
        )

    def from_mid(i):
        return pltpu.make_async_remote_copy(
            src_ref=mid.at[i - 4],
            dst_ref=xb.at[:, (1 - x_hi) * 4 + z, core],
            send_sem=mid_out.at[i - 4],
            recv_sem=recv_sem.at[i],
            device_id=along(i - 4),
            device_id_type=MESH,
        )

    def landed(i):
        return send(i) if i <= 4 else from_mid(i)

    def forward(i):
        chip = from_chip(i)
        return pltpu.make_async_remote_copy(
            src_ref=xb.at[:, chip, core],
            dst_ref=xb.at[:, chip, core],
            send_sem=pass_sem.at[i],
            recv_sem=passed_sem.at[i],
            device_id=sibling,
            device_id_type=MESH,
        )

    relayout(SENDS[0])
    pl.semaphore_wait(barrier, len(peers))
    to_mid(SENDS[0]).start()

    def relayout_and_send(j, carry):
        i = pick(SENDS, j)
        relayout(i)

        @pl.when(i > 4)
        def _():
            to_mid(i).start()

        @pl.when(i <= 4)
        def _():
            send(i).start()

        return carry

    lax.fori_loop(1, chips - 1, relayout_and_send, 0)
    load(0).wait()

    def put_own(b, r, part, value):
        xb[b, me, core, r : r + 16, part * half : (part + 1) * half] = value

    transposed(0, put_own)
    forward(0).start()

    lane = lax.broadcasted_iota(jnp.int32, (2 * own, 128), 1)

    def normalise(i):
        forward(i).wait_recv()
        chip = from_chip(i)
        power = jnp.ones((2 * own, 128), jnp.float32)
        for b in range(bands):
            v = xb[b, chip].reshape(2 * own, depth).astype(jnp.float32)
            v = v * v
            total = jnp.sum(v[:, :half] + v[:, half:], axis=1, keepdims=True) + epsilon
            power = jnp.where(lane == b, total, power)
        inverse = 1.0 / power
        inv_col[pl.ds(pl.multiple_of(chip * 2 * own, 128), 2 * own), :] = inverse
        inv_row[:, pl.ds(pl.multiple_of(chip * 128, 128), 128)] = inverse.T[:8, :]

    contract = (((1,), (1,)), ((), ()))
    stores = ((pa, 0), (pb, 1), (pc, 2))
    at = {"x": x, "y": y, "z": z}

    def target(dim, there):
        place = dict(at)
        place[dim] = there
        return device(place["x"], place["y"], place["z"], core)

    def hop(n, phase, o, cut=()):
        dim = PARTS[n][2][phase]
        there = (at[dim] + o) % 4
        src = stores[n][0]
        for d in PARTS[n][2][:phase]:
            src = src.at[at[d]]
        src = src.at[there]
        dst = ((ra1, rb1, rc1), (ra2, rb2, rc2), (ra3, rb3, rc3))[phase][n].at[o - 1]
        if cut:
            src, dst = src.at[cut], dst.at[cut]
        return pltpu.make_async_remote_copy(
            src_ref=src,
            dst_ref=dst,
            send_sem=out_sem.at[n, phase, o],
            recv_sem=in_sem.at[n, phase, o],
            device_id=target(dim, there),
            device_id_type=MESH,
        )

    def group(items):
        def one(j, carry):
            normalise(pick(items, j))
            return carry

        lax.fori_loop(0, len(items), one, 0)

    for event in EVENTS:
        if isinstance(event, tuple):
            group(event)
        elif event < 0:
            to_mid(-event).wait_recv()
            from_mid(-event).start()
        else:
            landed(event).wait_recv()
            forward(event).start()

    def tile(t, carry):
        row = (x_hi + 1 + t // 4) % 2
        col = (y + 2 + 3 * (t % 4)) % 4
        acc = jnp.zeros((256, 256), jnp.float32)
        scale_row = inv_row[:, pl.ds(pl.multiple_of(col * 256, 256), 256)]
        for b in range(bands):
            left = xb[b, pl.ds(row * 4, 4), core].reshape(256, depth)
            right = xb[b, pl.ds(col * 2, 2)].reshape(256, depth)
            turned = jnp.concatenate([left[:, half:], -left[:, :half]], axis=1)
            re = lax.dot_general(left, right, contract, preferred_element_type=jnp.float32)
            im = lax.dot_general(turned, right, contract, preferred_element_type=jnp.float32)
            rows = jnp.concatenate(
                [
                    inv_col[pl.ds(pl.multiple_of((row * 4 + q) * 128 + core * own, own), own), b : b + 1]
                    for q in range(4)
                ],
                axis=0,
            )
            acc += ((re * re + im * im) * rows) * scale_row[b : b + 1, :]
        for q in range(4):
            for s in range(2):
                for ref, n in stores:
                    low, high, order = PARTS[n]
                    place = {"x": row * 2 + s, "y": col, "z": q}
                    ref[tuple(place[d] for d in order)] = acc[q * 64 + low : q * 64 + high, s * 128 : (s + 1) * 128]
        for o in range(1, 4):
            x_to = (x + o) % 4

            @pl.when(x_to // 2 == row)
            def _():
                hop(0, 0, o, (col,)).start()

            @pl.when((y + o) % 4 == col)
            def _():
                hop(1, 0, o, (slice(None), pl.ds(row * 2, 2))).start()

            hop(2, 0, o, (pl.ds(row * 2, 2), col)).start()
        return carry

    lax.fori_loop(0, 8, tile, 0)

    for phase in range(3):
        for n in range(3):
            low, high, order = PARTS[n]
            got = ((ra1, rb1, rc1), (ra2, rb2, rc2), (ra3, rb3, rc3))[phase][n]
            for o in (1, 3, 2):
                hop(n, phase, o).wait_recv()
            index = tuple(at[d] for d in order[: phase + 1])
            total = (stores[n][0][index] + got[0]) + (got[1] + got[2])
            if phase < 2:
                stores[n][0][index] = total
                for o in (2, 1, 3):
                    hop(n, phase + 1, o).start()
            else:
                groups = lax.axis_size("band")
                scale = jnp.float32(W * tapers / (bands * chips * groups))
                row = lax.broadcasted_iota(jnp.int32, (high - low, 128), 0) + (chan * own + low)
                col = lax.broadcasted_iota(jnp.int32, (high - low, 128), 1) + band * 128
                out_ref[low:high, :] = jnp.where(row == col, jnp.float32(0.0), total) * scale

    for n in range(3):
        for phase in range(3):
            for o in (1, 2, 3):
                hop(n, phase, o).wait_send()
    for i in range(1, 8):
        (to_mid(i) if i > 4 else send(i)).wait_send()
        forward(i).wait_send()
        if i > 4:
            from_mid(i).wait_send()
    forward(0).wait_send()


def body(coeffs):
    parts, tapers, own, bins = coeffs.shape
    chips = lax.axis_size("chan") // 2
    bands = 128 // W
    depth = parts * tapers * W
    rows = [high - low for low, high, _ in PARTS]
    f32 = jnp.float32
    bf16 = jnp.bfloat16
    scratch = [
        pltpu.VMEM((chips, parts, tapers, own, 128), bf16),
        pltpu.VMEM((chips, bands, own, depth), bf16),
        pltpu.VMEM((4, bands, own, depth), bf16),
        pltpu.VMEM((bands, chips, 2, own, depth), bf16),
        pltpu.VMEM((chips * 2 * own, 128), f32),
        pltpu.VMEM((8, chips * 2 * own), f32),
    ]
    scratch += [pltpu.VMEM((4, 4, 4, r, 128), f32) for r in rows]
    scratch += [pltpu.VMEM((3, 4, 4, r, 128), f32) for r in rows]
    scratch += [pltpu.VMEM((3, 4, r, 128), f32) for r in rows]
    scratch += [pltpu.VMEM((3, r, 128), f32) for r in rows]
    scratch += [
        pltpu.SemaphoreType.DMA((chips,)),
        pltpu.SemaphoreType.DMA((chips,)),
        pltpu.SemaphoreType.DMA((chips,)),
        pltpu.SemaphoreType.DMA((4,)),
        pltpu.SemaphoreType.DMA((4,)),
        pltpu.SemaphoreType.DMA((chips,)),
        pltpu.SemaphoreType.DMA((chips,)),
        pltpu.SemaphoreType.DMA((3, 3, 4)),
        pltpu.SemaphoreType.DMA((3, 3, 4)),
    ]
    return pl.pallas_call(
        kernel,
        out_shape=jax.ShapeDtypeStruct((own, 128), f32),
        in_specs=[pl.BlockSpec(memory_space=pl.ANY)],
        out_specs=pl.BlockSpec(memory_space=pltpu.VMEM),
        scratch_shapes=scratch,
        compiler_params=pltpu.CompilerParams(
            collective_id=0, has_side_effects=True, vmem_limit_bytes=54000 * 1024
        ),
    )(coeffs)


def solution(mesh):
    return jax.shard_map(
        body,
        mesh=mesh,
        in_specs=(P(None, None, "chan", "band"),),
        out_specs=P("chan", "band"),
        check_vma=False,
    )
```

```python
import jax
import jax.numpy as jnp
from jax import lax
from jax.experimental import pallas as pl
from jax.experimental.pallas import tpu as pltpu
from jax.sharding import PartitionSpec as P

W = 16

SENDS = (6, 2, 5, 1, 7, 3, 4)
EVENTS = (-6, 2, -5, 1, 3, (0, 2, 1, 3), -7, 6, 5, 7, 4, (6, 5, 7, 4))

epsilon = 1e-06

MESH = pl.DeviceIdType.MESH

PARTS = ((0, 24, "xyz"), (24, 40, "yzx"), (40, 64, "zxy"))


def kernel(
    x_ref, out_ref, win, snd, mid, xb, inv_col, inv_row, pa, pb, pc, ra1, rb1, rc1, ra2, rb2, rc2, ra3, rb3, rc3,
    load_sem, send_sem, recv_sem, mid_in, mid_out, pass_sem, passed_sem, out_sem, in_sem,
):
    band = lax.axis_index("band")
    chan = lax.axis_index("chan")
    core = chan % 2
    z = (chan // 2) % 4
    x_hi = chan // 8
    y = band // 2
    x = x_hi * 2 + band % 2
    me = x_hi * 4 + z
    bands, chips, cores, own, depth = xb.shape
    half = depth // 2
    tapers = half // W

    def device(x, y, z, core):
        return {"band": y * 2 + x % 2, "chan": ((x // 2) * 4 + z) * 2 + core}

    def pick(table, j):
        return sum(v * (1 - jnp.minimum(jnp.abs(j - n), 1)) for n, v in enumerate(table))

    def to_chip(i):
        return ((x_hi + i // 4) % 2) * 4 + (z + i % 4) % 4

    def from_chip(i):
        return ((x_hi + 2 - i // 4) % 2) * 4 + (z + 4 - i % 4) % 4

    def same_group(chip):
        return {"band": band, "chan": chip * 2 + core}

    sibling = {"band": band, "chan": me * 2 + 1 - core}

    barrier = pltpu.get_barrier_semaphore()
    peers = [sibling] + [device((x + o) % 4, y, z, core) for o in (1, 2, 3)]
    peers += [device(x, (y + o) % 4, z, core) for o in (1, 2, 3)]
    peers += [device(x, y, (z + o) % 4, core) for o in (1, 2, 3)]
    for peer in peers:
        pl.semaphore_signal(barrier, inc=1, device_id=peer, device_id_type=MESH)

    def load(i):
        chip = to_chip(i)
        lanes = pl.ds(pl.multiple_of(chip * 128, 128), 128)
        return pltpu.make_async_copy(x_ref.at[:, :, :, lanes], win.at[i], load_sem.at[i])

    for i in SENDS + (0,):
        load(i).start()

    lane_band = lax.broadcasted_iota(jnp.int32, (16, 128), 1) // W

    def transposed(i, put):
        for part in range(2):
            for r in range(0, own, 16):
                v = [win[i, part, k, r : r + 16, :].astype(jnp.float32) for k in range(tapers)]
                bit = 1
                while bit < tapers:
                    upper = (lane_band // bit) % 2 == 1
                    for a in range(tapers):
                        if not a & bit:
                            b = a | bit
                            up = pltpu.roll(v[b], W * bit, 1)
                            down = pltpu.roll(v[a], 128 - W * bit, 1)
                            v[a], v[b] = jnp.where(upper, up, v[a]), jnp.where(upper, v[b], down)
                    bit *= 2
                for b in range(bands):
                    put(b, r, part, v[b].astype(jnp.bfloat16))

    def relayout(i):
        load(i).wait()

        def put(b, r, part, value):
            snd[i, b, r : r + 16, part * half : (part + 1) * half] = value

        transposed(i, put)

    across = device((x + 2) % 4, y, z, core)

    def along(dz):
        return device(x, y, (z + dz) % 4, core)

    def send(i):
        return pltpu.make_async_remote_copy(
            src_ref=snd.at[i],
            dst_ref=xb.at[:, me, core],
            send_sem=send_sem.at[i],
            recv_sem=recv_sem.at[i],
            device_id=device((x + 2 * (i // 4)) % 4, y, (z + i % 4) % 4, core),
            device_id_type=MESH,
        )

    def to_mid(i):
        return pltpu.make_async_remote_copy(
            src_ref=snd.at[i],
            dst_ref=mid.at[i - 4],
            send_sem=send_sem.at[i],
            recv_sem=mid_in.at[i - 4],
            device_id=across,
            device_id_type=MESH,
        )

    def from_mid(i):
        return pltpu.make_async_remote_copy(
            src_ref=mid.at[i - 4],
            dst_ref=xb.at[:, (1 - x_hi) * 4 + z, core],
            send_sem=mid_out.at[i - 4],
            recv_sem=recv_sem.at[i],
            device_id=along(i - 4),
            device_id_type=MESH,
        )

    def landed(i):
        return send(i) if i <= 4 else from_mid(i)

    def forward(i):
        chip = from_chip(i)
        return pltpu.make_async_remote_copy(
            src_ref=xb.at[:, chip, core],
            dst_ref=xb.at[:, chip, core],
            send_sem=pass_sem.at[i],
            recv_sem=passed_sem.at[i],
            device_id=sibling,
            device_id_type=MESH,
        )

    relayout(SENDS[0])
    pl.semaphore_wait(barrier, len(peers))
    to_mid(SENDS[0]).start()

    def relayout_and_send(j, carry):
        i = pick(SENDS, j)
        relayout(i)

        @pl.when(i > 4)
        def _():
            to_mid(i).start()

        @pl.when(i <= 4)
        def _():
            send(i).start()

        return carry

    lax.fori_loop(1, chips - 1, relayout_and_send, 0)
    load(0).wait()

    def put_own(b, r, part, value):
        xb[b, me, core, r : r + 16, part * half : (part + 1) * half] = value

    transposed(0, put_own)
    forward(0).start()

    lane = lax.broadcasted_iota(jnp.int32, (2 * own, 128), 1)

    def normalise(i):
        forward(i).wait_recv()
        chip = from_chip(i)
        power = jnp.ones((2 * own, 128), jnp.float32)
        for b in range(bands):
            v = xb[b, chip].reshape(2 * own, depth).astype(jnp.float32)
            v = v * v
            total = jnp.sum(v[:, :half] + v[:, half:], axis=1, keepdims=True) + epsilon
            power = jnp.where(lane == b, total, power)
        inverse = 1.0 / power
        inv_col[pl.ds(pl.multiple_of(chip * 2 * own, 128), 2 * own), :] = inverse
        inv_row[:, pl.ds(pl.multiple_of(chip * 128, 128), 128)] = inverse.T[:8, :]

    contract = (((1,), (1,)), ((), ()))
    stores = ((pa, 0), (pb, 1), (pc, 2))
    at = {"x": x, "y": y, "z": z}

    def target(dim, there):
        place = dict(at)
        place[dim] = there
        return device(place["x"], place["y"], place["z"], core)

    def hop(n, phase, o, cut=()):
        dim = PARTS[n][2][phase]
        there = (at[dim] + o) % 4
        src = stores[n][0]
        for d in PARTS[n][2][:phase]:
            src = src.at[at[d]]
        src = src.at[there]
        dst = ((ra1, rb1, rc1), (ra2, rb2, rc2), (ra3, rb3, rc3))[phase][n].at[o - 1]
        if cut:
            src, dst = src.at[cut], dst.at[cut]
        return pltpu.make_async_remote_copy(
            src_ref=src,
            dst_ref=dst,
            send_sem=out_sem.at[n, phase, o],
            recv_sem=in_sem.at[n, phase, o],
            device_id=target(dim, there),
            device_id_type=MESH,
        )

    def group(items):
        def one(j, carry):
            normalise(pick(items, j))
            return carry

        lax.fori_loop(0, len(items), one, 0)

    for event in EVENTS:
        if isinstance(event, tuple):
            group(event)
        elif event < 0:
            to_mid(-event).wait_recv()
            from_mid(-event).start()
        else:
            landed(event).wait_recv()
            forward(event).start()

    def tile(t, carry):
        row = (x_hi + 1 + t // 4) % 2
        col = (y + 2 + 3 * (t % 4)) % 4
        acc = jnp.zeros((256, 256), jnp.float32)
        scale_row = inv_row[:, pl.ds(pl.multiple_of(col * 256, 256), 256)]
        for b in range(bands):
            left = xb[b, pl.ds(row * 4, 4), core].reshape(256, depth)
            right = xb[b, pl.ds(col * 2, 2)].reshape(256, depth)
            turned = jnp.concatenate([left[:, half:], -left[:, :half]], axis=1)
            re = lax.dot_general(left, right, contract, preferred_element_type=jnp.float32)
            im = lax.dot_general(turned, right, contract, preferred_element_type=jnp.float32)
            rows = jnp.concatenate(
                [
                    inv_col[pl.ds(pl.multiple_of((row * 4 + q) * 128 + core * own, own), own), b : b + 1]
                    for q in range(4)
                ],
                axis=0,
            )
            acc += ((re * re + im * im) * rows) * scale_row[b : b + 1, :]
        for q in range(4):
            for s in range(2):
                for ref, n in stores:
                    low, high, order = PARTS[n]
                    place = {"x": row * 2 + s, "y": col, "z": q}
                    ref[tuple(place[d] for d in order)] = acc[q * 64 + low : q * 64 + high, s * 128 : (s + 1) * 128]
        for o in range(1, 4):
            x_to = (x + o) % 4

            @pl.when(x_to // 2 == row)
            def _():
                hop(0, 0, o, (col,)).start()

            @pl.when((y + o) % 4 == col)
            def _():
                hop(1, 0, o, (slice(None), pl.ds(row * 2, 2))).start()

            hop(2, 0, o, (pl.ds(row * 2, 2), col)).start()
        return carry

    def two_tiles(t, carry):
        tile(2 * t, 0)
        tile(2 * t + 1, 0)
        return carry

    lax.fori_loop(0, 4, two_tiles, 0)

    for phase in range(3):
        for n in range(3):
            low, high, order = PARTS[n]
            got = ((ra1, rb1, rc1), (ra2, rb2, rc2), (ra3, rb3, rc3))[phase][n]
            for o in (1, 3, 2):
                hop(n, phase, o).wait_recv()
            index = tuple(at[d] for d in order[: phase + 1])
            total = (stores[n][0][index] + got[0]) + (got[1] + got[2])
            if phase < 2:
                stores[n][0][index] = total
                for o in (2, 1, 3):
                    hop(n, phase + 1, o).start()
            else:
                groups = lax.axis_size("band")
                scale = jnp.float32(W * tapers / (bands * chips * groups))
                row = lax.broadcasted_iota(jnp.int32, (high - low, 128), 0) + (chan * own + low)
                col = lax.broadcasted_iota(jnp.int32, (high - low, 128), 1) + band * 128
                out_ref[low:high, :] = jnp.where(row == col, jnp.float32(0.0), total) * scale

    for n in range(3):
        for phase in range(3):
            for o in (1, 2, 3):
                hop(n, phase, o).wait_send()
    for i in range(1, 8):
        (to_mid(i) if i > 4 else send(i)).wait_send()
        forward(i).wait_send()
        if i > 4:
            from_mid(i).wait_send()
    forward(0).wait_send()


def body(coeffs):
    parts, tapers, own, bins = coeffs.shape
    chips = lax.axis_size("chan") // 2
    bands = 128 // W
    depth = parts * tapers * W
    rows = [high - low for low, high, _ in PARTS]
    f32 = jnp.float32
    bf16 = jnp.bfloat16
    scratch = [
        pltpu.VMEM((chips, parts, tapers, own, 128), bf16),
        pltpu.VMEM((chips, bands, own, depth), bf16),
        pltpu.VMEM((4, bands, own, depth), bf16),
        pltpu.VMEM((bands, chips, 2, own, depth), bf16),
        pltpu.VMEM((chips * 2 * own, 128), f32),
        pltpu.VMEM((8, chips * 2 * own), f32),
    ]
    scratch += [pltpu.VMEM((4, 4, 4, r, 128), f32) for r in rows]
    scratch += [pltpu.VMEM((3, 4, 4, r, 128), f32) for r in rows]
    scratch += [pltpu.VMEM((3, 4, r, 128), f32) for r in rows]
    scratch += [pltpu.VMEM((3, r, 128), f32) for r in rows]
    scratch += [
        pltpu.SemaphoreType.DMA((chips,)),
        pltpu.SemaphoreType.DMA((chips,)),
        pltpu.SemaphoreType.DMA((chips,)),
        pltpu.SemaphoreType.DMA((4,)),
        pltpu.SemaphoreType.DMA((4,)),
        pltpu.SemaphoreType.DMA((chips,)),
        pltpu.SemaphoreType.DMA((chips,)),
        pltpu.SemaphoreType.DMA((3, 3, 4)),
        pltpu.SemaphoreType.DMA((3, 3, 4)),
    ]
    return pl.pallas_call(
        kernel,
        out_shape=jax.ShapeDtypeStruct((own, 128), f32),
        in_specs=[pl.BlockSpec(memory_space=pl.ANY)],
        out_specs=pl.BlockSpec(memory_space=pltpu.VMEM),
        scratch_shapes=scratch,
        compiler_params=pltpu.CompilerParams(
            collective_id=0, has_side_effects=True, vmem_limit_bytes=54000 * 1024
        ),
    )(coeffs)


def solution(mesh):
    return jax.shard_map(
        body,
        mesh=mesh,
        in_specs=(P(None, None, "chan", "band"),),
        out_specs=P("chan", "band"),
        check_vma=False,
    )
```
